32 devices in a mesh: ka: 8 (over y, x, core), ga: 4 (over z).
Axes of the slice: x: 2, y: 2, z: 4, core: 2. Of those that a mesh axis runs over, the one named last changes fastest.
Arguments:
- coeffs: bfloat16 [8, 2, 7680, 256], P('ka', None, 'ga'), may hold values from -1 to 1
- projectors: bfloat16 [2, 7680, 1024], P(None, 'ga'), may hold values from -1.5 to 1.5
- proj_deriv: bfloat16 [2, 7680, 1024], P(None, 'ga'), may hold values from -1.5 to 1.5
- shift_map: int32 [7680], P('ga'), may hold values from 0 to 7679, as said below
- atom_of: int32 [1024], replicated, may hold values from 0 to 127, as said below
Outputs:
- transport: float32 [8, 2, 256, 256], P('ka')
- forces: float32 [128], replicated
The draws below stay inside these ranges and needn't reach their ends.
Inputs may be any that keep to these rules, and one draw needn't show every extreme that they name: `shift_map`: a permutation that maps each aligned block of 1920 plane waves onto itself. `atom_of`: each atom owns exactly 8 projectors.
All inputs are finite; a program needn't handle non-finite values.
Results may differ from the reference program's by a relative error of at most 0.0003.
Values may be sent and summed in bfloat16 or wider, within the bound.
A program may use at most 128 MiB of HBM per device.

```python
import math
import jax
import jax.numpy as jnp
from jax import lax

NB = 256
GD = 1920
NP = 1024
NA = 128
NEWTON = 2
NK = 8
NG = 7680


def block_shift(key):
    start_key = jax.random.fold_in(key, 11)
    block_keys = jax.random.split(start_key, NG // GD)
    shuffled = jax.vmap(lambda single: jax.random.permutation(single, GD))(block_keys)
    offsets = jnp.arange(NG // GD, dtype=jnp.int32) * GD
    return (shuffled.astype(jnp.int32) + offsets[:, None]).reshape(NG)


def draw_shift_map(key, part):
    return block_shift(key)


def draw_coeffs(key, part):
    mapping = block_shift(key)
    common_key = jax.random.fold_in(key, 21)
    spread_key = jax.random.fold_in(key, 22)
    common = jax.random.normal(common_key, (2, NG, NB), jnp.float32)
    spread_part = 0.3 * jax.random.normal(spread_key, (NK, 2, NG, NB), jnp.float32)
    norming = (2.0 * NG) ** (-0.5)
    common = common * norming
    spread_part = spread_part * norming
    angles = math.pi / 2 * jnp.arange(NK, dtype=jnp.float32) / NK
    moved = common[:, mapping, :]
    values = jnp.cos(angles)[:, None, None, None] * common[None] + jnp.sin(angles)[:, None, None, None] * moved[None] + spread_part
    return jnp.clip(values, -1.0, 1.0).astype(jnp.bfloat16)


def draw_atom_of(key, part):
    order = jax.random.permutation(jax.random.fold_in(key, 31), NP)
    return (order // (NP // NA)).astype(jnp.int32)


def level_of(stream_key, extent, pieces, smallest, top_value):
    def one(dim, parts):
        heights = jax.random.uniform(jax.random.fold_in(jax.random.fold_in(stream_key, 6), dim), (parts,), jnp.float32, smallest / len(pieces), top_value / len(pieces))
        return jnp.repeat(jnp.exp(heights), extent[dim] // parts).reshape((-1,) + (1,) * (len(extent) - dim - 1))

    factor_of = one(*pieces[0])
    for cut in pieces[1:]:
        factor_of = factor_of * one(*cut)
    return factor_of


def gaussian(stream_key, extent, scale, bound, pieces=(), kind=jnp.bfloat16):
    drawn = jax.random.normal(stream_key, extent, jnp.float32) * scale
    if len(pieces) > 0:
        drawn = level_of(stream_key, extent, pieces, -0.22, 0.18) * drawn
    return jnp.clip(drawn, min=-bound, max=bound).astype(kind)


def setup_inputs(seed: int = 0) -> dict:
    arg_keys = jax.random.split(jax.random.key(seed), 6)
    return {
        "coeffs": draw_coeffs(jax.random.fold_in(arg_keys[5], 71), 0),
        "projectors": gaussian(arg_keys[1], (2, NG, NP), 0.25, 1.5, ((1, 4),)),
        "proj_deriv": gaussian(arg_keys[2], (2, NG, NP), 0.25, 1.5, ((1, 4),)),
        "shift_map": draw_shift_map(jax.random.fold_in(arg_keys[5], 71), 0),
        "atom_of": draw_atom_of(jax.random.fold_in(arg_keys[5], 71), 0),
    }


def cmul(left, right):
    highest = lax.Precision.HIGHEST
    left_re, left_im = left[..., 0, :, :], left[..., 1, :, :]
    right_re, right_im = right[..., 0, :, :], right[..., 1, :, :]
    real_part = jnp.matmul(left_re, right_re, precision=highest) - jnp.matmul(left_im, right_im, precision=highest)
    imag_part = jnp.matmul(left_re, right_im, precision=highest) + jnp.matmul(left_im, right_re, precision=highest)
    return jnp.stack([real_part, imag_part], axis=-3)


def invert(intersection, eye_c):
    estimate = eye_c
    for newton_step in range(NEWTON):
        estimate = cmul(estimate, 2.0 * eye_c - cmul(intersection, estimate))
    return estimate


def project(proj_table, columns, swapped):
    real_part = jnp.dot(proj_table.T, columns, preferred_element_type=jnp.float32)
    imag_part = jnp.dot(proj_table.T, swapped, preferred_element_type=jnp.float32)
    return jnp.stack([real_part, imag_part])


def reference(coeffs, projectors, proj_deriv, shift_map, atom_of):
    proj_table = projectors.reshape(2 * NG, NP)
    deriv_table = proj_deriv.reshape(2 * NG, NP)
    eye_c = jnp.stack([jnp.eye(NB, dtype=jnp.float32), jnp.zeros((NB, NB), jnp.float32)])

    def k_point(state_pair, k_index):
        running, accumulated = state_pair
        own_point = lax.dynamic_index_in_dim(coeffs, k_index, 0, keepdims=False)
        following = lax.dynamic_index_in_dim(coeffs, (k_index + 1) % NK, 0, keepdims=False)
        following = jnp.where(k_index == NK - 1, following[:, shift_map, :], following)
        columns = own_point.reshape(2 * NG, NB)
        own_swap = jnp.concatenate([own_point[1], -own_point[0]], axis=0)
        next_cols = following.reshape(2 * NG, NB)
        next_swap = jnp.concatenate([following[1], -following[0]], axis=0)
        intersections = jnp.stack([
            jnp.dot(columns.T, next_cols, preferred_element_type=jnp.float32),
            jnp.dot(columns.T, next_swap, preferred_element_type=jnp.float32)])
        inverse = invert(intersections, eye_c)
        running = cmul(running, inverse)
        proj_vals = project(proj_table, columns, own_swap)
        deriv_vals = project(deriv_table, columns, own_swap)
        weighted = cmul(proj_vals, running)
        accumulated = accumulated + jnp.sum(deriv_vals[0] * weighted[1] - deriv_vals[1] * weighted[0], axis=1)
        return (running, accumulated), running

    (running, accumulated), transport = lax.scan(
        k_point, (eye_c, jnp.zeros((NP,), jnp.float32)), jnp.arange(NK, dtype=jnp.int32))
    onehot = (atom_of[None, :] == jnp.arange(NA, dtype=jnp.int32)[:, None]).astype(jnp.float32)
    forces = jnp.dot(onehot, accumulated / NK, precision=lax.Precision.HIGHEST)
    return transport, forces
```

```python
import functools

import jax
import jax.numpy as jnp
from jax import lax
from jax.experimental import pallas as pl
from jax.experimental.pallas import tpu as pltpu
from jax.sharding import PartitionSpec as P

NA = 128
NEWTON = 2
F32 = jnp.float32
BF16 = jnp.bfloat16


def mm(left, right):
    return jnp.dot(left, right, precision=lax.Precision.HIGHEST, preferred_element_type=F32)


def cmul(lr, li, rr, ri):
    return mm(lr, rr) - mm(li, ri), mm(lr, ri) + mm(li, rr)


def kernel(
    nk, ng,
    c_hbm, p_hbm, d_hbm, map_ref, atom_ref,
    t_out, f_out,
    cv, nv, pv, lt, mp, mr, mfull, qs, scs, qr, scr, bown, tb, rb, fk, fg,
    c_sem, p_sem, sh_s, sh_r, m_s, m_r, a_s, a_r, q_s, q_r, x_s, x_r, f_s, f_r, g_s, g_r,
):
    k = lax.axis_index("ka")
    g = lax.axis_index("ga")
    rows = cv.shape[1]
    bands = cv.shape[2]
    share = pv.shape[3]
    piece = 2 * bands // ng
    even = k % 2 == 0
    odd = k % 2 == 1

    def remote(src, dst, ssem, rsem, to_k, to_g):
        return pltpu.make_async_remote_copy(
            src_ref=src, dst_ref=dst, send_sem=ssem, recv_sem=rsem,
            device_id=(to_k, to_g), device_id_type=pl.DeviceIdType.MESH,
        )

    load_c = pltpu.make_async_copy(c_hbm.at[0], cv, c_sem)
    load_c.start()

    def load(j, which):
        src = (p_hbm, d_hbm)[which]
        cols = pl.ds(pl.multiple_of(j * share, 128), share)
        return pltpu.make_async_copy(src.at[:, :, cols], pv.at[2 * j + which], p_sem.at[2 * j + which])

    for j in range(ng):
        load(j, 0).start()
        load(j, 1).start()

    barrier = pltpu.get_barrier_semaphore()
    for d in range(1, nk):
        pl.semaphore_signal(barrier, inc=1, device_id=((k + d) % nk, g), device_id_type=pl.DeviceIdType.MESH)
    for d in range(1, ng):
        pl.semaphore_signal(barrier, inc=1, device_id=(k, (g + d) % ng), device_id_type=pl.DeviceIdType.MESH)
    pl.semaphore_wait(barrier, nk + ng - 2)

    load_c.wait()
    shift = remote(cv, nv, sh_s, sh_r, (k + nk - 1) % nk, g)
    shift.start()

    def transpose_in(source):
        def body(i, carry):
            for half in range(2):
                at = pl.ds(pl.multiple_of(i * 128, 128), 128)
                block = source[half, at, :].T
                here = pl.ds(pl.multiple_of(half * rows + i * 128, 128), 128)
                there = pl.ds(pl.multiple_of((1 - half) * rows + i * 128, 128), 128)
                lt[0:bands, here] = block
                lt[bands:, there] = block if half == 1 else -block
            return carry
        lax.fori_loop(0, rows // 128, body, 0)

    transpose_in(cv)

    def m_copy(d):
        j = (g + d) % ng
        part = mp.at[pl.ds(pl.multiple_of(j * piece, 8), piece)]
        return remote(part, mr.at[g], m_s.at[d], m_r.at[g], k, j)

    def a_copy(d):
        j = (g + d) % ng
        part = mfull.at[pl.ds(pl.multiple_of(g * piece, 8), piece)]
        return remote(part, part, a_s.at[d], a_r.at[g], k, j)

    def m_partial():
        shift.wait_recv()
        mp[...] = jnp.dot(lt[...], nv[...].reshape(2 * rows, bands), preferred_element_type=F32)
        for d in range(1, ng):
            m_copy(d).start()

    def m_sum():
        own = pl.ds(pl.multiple_of(g * piece, 8), piece)
        total = mp[own]
        for d in range(1, ng):
            s = (g + d) % ng
            remote(mr.at[s], mr.at[s], m_s.at[d], m_r.at[s], k, s).wait_recv()
            total = total + mr[s]
        mfull[own] = total
        for d in range(1, ng):
            a_copy(d).start()

    def q_copies(d):
        j = (g + d) % ng
        return (
            remote(qs.at[j], qr.at[g], q_s.at[0, d], q_r.at[0, g], k, j),
            remote(scs.at[j], scr.at[g], q_s.at[1, d], q_r.at[1, g], k, j),
        )

    def q_start():
        for d in range(1, ng):
            for copy in q_copies(d):
                copy.start()

    @pl.when(even)
    def _():
        m_partial()

    def project(j, carry):
        for which in range(2):
            load(j, which).wait()
            table = pv[2 * j + which].reshape(2 * rows, share)
            res = jnp.dot(lt[...], table, preferred_element_type=F32)
            top = jnp.maximum(jnp.max(jnp.abs(res), axis=0, keepdims=True), 1e-30)
            coded = jnp.round(res * (32767.0 / top)).astype(jnp.int32)
            qs[j, which] = coded.astype(jnp.int16)
            scs[j, which] = jnp.broadcast_to(top * (1.0 / 32767.0), (8, share))

            @pl.when(j == g)
            def _():
                bown[which] = res
        return carry

    lax.fori_loop(0, ng, project, 0)

    @pl.when(even)
    def _():
        m_sum()
        q_start()

    @pl.when(k == nk - 1)
    def _():
        local = map_ref[...] % rows
        both = jnp.concatenate([cv[0], cv[1]], axis=1)

        def permute(i, carry):
            ids = lax.broadcasted_iota(jnp.int32, (128, rows), 0) + i * 128
            pick = jnp.where(ids == local, 1.0, 0.0).astype(BF16)
            moved = jnp.dot(pick, both, preferred_element_type=F32).astype(BF16)
            at = pl.ds(pl.multiple_of(i * 128, 128), 128)
            for half in range(2):
                block = moved[:, half * bands:(half + 1) * bands].T
                here = pl.ds(pl.multiple_of(half * rows + i * 128, 128), 128)
                there = pl.ds(pl.multiple_of((1 - half) * rows + i * 128, 128), 128)
                lt[0:bands, here] = block
                lt[bands:, there] = block if half == 1 else -block
            return carry

        lax.fori_loop(0, rows // 128, permute, 0)

    @pl.when(odd)
    def _():
        m_partial()
        m_sum()
        q_start()

    for d in range(1, ng):
        s = (g + d) % ng
        part = mfull.at[pl.ds(pl.multiple_of(s * piece, 8), piece)]
        remote(part, part, a_s.at[d], a_r.at[s], k, s).wait_recv()

    mre = mfull[0:bands]
    mim = -mfull[bands:]
    diagonal = lax.broadcasted_iota(jnp.int32, (bands, bands), 0) == lax.broadcasted_iota(
        jnp.int32, (bands, bands), 1
    )
    two = jnp.where(diagonal, 2.0, 0.0).astype(F32)
    xr, xi = two - mre, -mim
    for newton_step in range(NEWTON - 1):
        yr, yi = cmul(mre, mim, xr, xi)
        xr, xi = cmul(xr, xi, two - yr, -yi)
    tb[0, 0] = xr
    tb[0, 1] = xi

    step = 0
    width = 1
    while width < nk:
        now, later = tb.at[step], tb.at[step + 1]
        spot = k % (2 * width)
        is_source = spot == width - 1
        is_target = spot >= width
        if width == 1:
            copy = remote(now, rb.at[step], x_s.at[step, 0], x_r.at[step, 0], (k + 1) % nk, g)

            @pl.when(is_source)
            def _():
                copy.start()
                copy.wait_send()

            @pl.when(is_target)
            def _():
                copy.wait_recv()
        else:
            far = [
                remote(now.at[d % 2], rb.at[step, d % 2], x_s.at[step, d], x_r.at[step, 0], (k + 1 + d) % nk, g)
                for d in range(width)
            ]

            @pl.when(is_source)
            def _():
                for copy in far:
                    copy.start()

            def swap(half, partner):
                mine = rb.at[step, half]
                far[half].wait_recv()
                copy = remote(mine, mine, x_s.at[step, 0], x_r.at[step, 1], partner, g)
                copy.start()
                other = rb.at[step, 1 - half]
                remote(other, other, x_s.at[step, 0], x_r.at[step, 1], partner, g).wait_recv()
                copy.wait_send()

            @pl.when(jnp.logical_and(is_target, even))
            def _():
                swap(0, (k + 1) % nk)

            @pl.when(jnp.logical_and(is_target, odd))
            def _():
                swap(1, (k + nk - 1) % nk)

            @pl.when(is_source)
            def _():
                for copy in far:
                    copy.wait_send()

        @pl.when(is_target)
        def _():
            vr, vi = cmul(rb[step, 0], rb[step, 1], now[0], now[1])
            later[0] = vr
            later[1] = vi

        @pl.when(jnp.logical_not(is_target))
        def _():
            later[...] = now[...]

        step += 1
        width *= 2

    tr, ti = tb[step, 0], tb[step, 1]
    t_out[0, 0] = tr
    t_out[0, 1] = ti

    sums = [bown[0], bown[1]]
    for d in range(1, ng):
        s = (g + d) % ng
        remote(qr.at[s], qr.at[s], q_s.at[0, d], q_r.at[0, s], k, s).wait_recv()
        remote(scr.at[s], scr.at[s], q_s.at[1, d], q_r.at[1, s], k, s).wait_recv()
        for which in range(2):
            scale = scr[s, which][0:1]
            sums[which] = sums[which] + qr[s, which].astype(jnp.int32).astype(F32) * scale
    br, bi = sums[0][0:bands], sums[0][bands:]
    dr, di = sums[1][0:bands], sums[1][bands:]
    wr, wi = cmul(tr.T, ti.T, br, bi)
    fp = jnp.sum(dr * wi - di * wr, axis=0, keepdims=True) * (1.0 / nk)
    atoms = atom_ref[pl.ds(g, 1), :]
    onehot = (lax.broadcasted_iota(jnp.int32, (NA, share), 0) == atoms).astype(F32)
    force = lax.dot_general(
        jnp.broadcast_to(fp, (8, share)), onehot, (((1,), (1,)), ((), ())),
        precision=lax.Precision.HIGHEST, preferred_element_type=F32,
    )

    fk[pl.ds(k, 1)] = force[None]
    for d in range(1, nk):
        remote(fk.at[k], fk.at[k], f_s.at[d], f_r.at[k], (k + d) % nk, g).start()
    for d in range(1, nk):
        s = (k + d) % nk
        remote(fk.at[s], fk.at[s], f_s.at[d], f_r.at[s], s, g).wait_recv()
    total = fk[0]
    for s in range(1, nk):
        total = total + fk[s]
    fg[pl.ds(g, 1)] = total[None]
    for d in range(1, ng):
        remote(fg.at[g], fg.at[g], g_s.at[d], g_r.at[g], k, (g + d) % ng).start()
    for d in range(1, ng):
        s = (g + d) % ng
        remote(fg.at[s], fg.at[s], g_s.at[d], g_r.at[s], k, s).wait_recv()
    total = fg[0]
    for s in range(1, ng):
        total = total + fg[s]
    f_out[...] = total

    shift.wait_send()
    for d in range(1, ng):
        m_copy(d).wait_send()
        a_copy(d).wait_send()
        for copy in q_copies(d):
            copy.wait_send()
        remote(fg.at[g], fg.at[g], g_s.at[d], g_r.at[g], k, (g + d) % ng).wait_send()
    for d in range(1, nk):
        remote(fk.at[k], fk.at[k], f_s.at[d], f_r.at[k], (k + d) % nk, g).wait_send()


def local(coeffs, projectors, proj_deriv, shift_map, atom_of):
    nk, ng = lax.axis_size("ka"), lax.axis_size("ga")
    rows, bands = coeffs.shape[2:]
    count = projectors.shape[2]
    share = count // ng
    steps = max(nk - 1, 1).bit_length()
    dma = pltpu.SemaphoreType.DMA
    vm = pl.BlockSpec(memory_space=pltpu.VMEM)
    hbm = pl.BlockSpec(memory_space=pl.ANY)
    transport, forces = pl.pallas_call(
        functools.partial(kernel, nk, ng),
        out_shape=(
            jax.ShapeDtypeStruct((1, 2, bands, bands), F32),
            jax.ShapeDtypeStruct((8, NA), F32),
        ),
        in_specs=[hbm, hbm, hbm, vm, vm],
        out_specs=(vm, vm),
        scratch_shapes=[
            pltpu.VMEM((2, rows, bands), BF16),
            pltpu.VMEM((2, rows, bands), BF16),
            pltpu.VMEM((2 * ng, 2, rows, share), BF16),
            pltpu.VMEM((2 * bands, 2 * rows), BF16),
            pltpu.VMEM((2 * bands, bands), F32),
            pltpu.VMEM((ng, 2 * bands // ng, bands), F32),
            pltpu.VMEM((2 * bands, bands), F32),
            pltpu.VMEM((ng, 2, 2 * bands, share), jnp.int16),
            pltpu.VMEM((ng, 2, 8, share), F32),
            pltpu.VMEM((ng, 2, 2 * bands, share), jnp.int16),
            pltpu.VMEM((ng, 2, 8, share), F32),
            pltpu.VMEM((2, 2 * bands, share), F32),
            pltpu.VMEM((steps + 1, 2, bands, bands), F32),
            pltpu.VMEM((steps, 2, bands, bands), F32),
            pltpu.VMEM((nk, 8, NA), F32),
            pltpu.VMEM((ng, 8, NA), F32),
            dma, dma((2 * ng,)), dma, dma,
            dma((ng,)), dma((ng,)), dma((ng,)), dma((ng,)),
            dma((2, ng)), dma((2, ng)),
            dma((steps, max(nk // 2, 2))), dma((steps, 2)),
            dma((nk,)), dma((nk,)), dma((ng,)), dma((ng,)),
        ],
        compiler_params=pltpu.CompilerParams(
            collective_id=0, has_side_effects=True, vmem_limit_bytes=60 * 1024 * 1024
        ),
    )(coeffs, projectors, proj_deriv, shift_map.reshape(1, rows), atom_of.reshape(ng, share))
    return transport, forces[0]


def solution(mesh):
    placed = (P("ka", None, "ga", None), P(None, "ga", None), P(None, "ga", None), P("ga"), P())
    return jax.shard_map(
        local,
        mesh=mesh,
        in_specs=placed,
        out_specs=(P("ka", None, None, None), P()),
        check_vma=False,
    )
```

```python
import functools

import jax
import jax.numpy as jnp
from jax import lax
from jax.experimental import pallas as pl
from jax.experimental.pallas import tpu as pltpu
from jax.sharding import PartitionSpec as P

NA = 128
NEWTON = 2
F32 = jnp.float32
BF16 = jnp.bfloat16


def mm(left, right):
    return jnp.dot(left, right, precision=lax.Precision.HIGHEST, preferred_element_type=F32)


def cmul(lr, li, rr, ri):
    return mm(lr, rr) - mm(li, ri), mm(lr, ri) + mm(li, rr)


def kernel(
    nk, ng,
    c_hbm, p_hbm, d_hbm, map_ref, atom_ref,
    t_out, f_out,
    cv, nv, pv, lt, mp, mr, mfull, qs, scs, qr, scr, qs2, scs2, qr2, scr2, own, tb, rb, fk, fg,
    c_sem, p_sem, sh_s, sh_r, m_s, m_r, a_s, a_r, q_s, q_r, q2_s, q2_r, x_s, x_r, f_s, f_r, g_s, g_r,
):
    k = lax.axis_index("ka")
    g = lax.axis_index("ga")
    rows = cv.shape[1]
    bands = cv.shape[2]
    share = pv.shape[3]
    piece = 2 * bands // ng
    even = k % 2 == 0
    odd = k % 2 == 1
    side = g % 2
    mate = g + 1 - 2 * side
    pair = g // 2
    pairs = ng // 2

    def remote(src, dst, ssem, rsem, to_k, to_g):
        return pltpu.make_async_remote_copy(
            src_ref=src, dst_ref=dst, send_sem=ssem, recv_sem=rsem,
            device_id=(to_k, to_g), device_id_type=pl.DeviceIdType.MESH,
        )

    load_c = pltpu.make_async_copy(c_hbm.at[0], cv, c_sem)
    load_c.start()

    def load(j, which):
        src = (p_hbm, d_hbm)[which]
        cols = pl.ds(pl.multiple_of(j * share, 128), share)
        return pltpu.make_async_copy(src.at[:, :, cols], pv.at[2 * j + which], p_sem.at[2 * j + which])

    def order(t):
        return 2 * (t % pairs) + jnp.where(t < pairs, 1 - side, side)

    for t in range(ng):
        load(order(t), 0).start()
        load(order(t), 1).start()

    barrier = pltpu.get_barrier_semaphore()
    for d in range(1, nk):
        pl.semaphore_signal(barrier, inc=1, device_id=((k + d) % nk, g), device_id_type=pl.DeviceIdType.MESH)
    for d in range(1, ng):
        pl.semaphore_signal(barrier, inc=1, device_id=(k, (g + d) % ng), device_id_type=pl.DeviceIdType.MESH)
    pl.semaphore_wait(barrier, nk + ng - 2)

    load_c.wait()
    shift = remote(cv, nv, sh_s, sh_r, (k + nk - 1) % nk, g)
    shift.start()

    def transpose_in(source):
        def body(i, carry):
            for half in range(2):
                at = pl.ds(pl.multiple_of(i * 128, 128), 128)
                block = source[half, at, :].T
                here = pl.ds(pl.multiple_of(half * rows + i * 128, 128), 128)
                there = pl.ds(pl.multiple_of((1 - half) * rows + i * 128, 128), 128)
                lt[0:bands, here] = block
                lt[bands:, there] = block if half == 1 else -block
            return carry
        lax.fori_loop(0, rows // 128, body, 0)

    transpose_in(cv)

    def m_copy(d):
        j = (g + d) % ng
        part = mp.at[pl.ds(pl.multiple_of(j * piece, 8), piece)]
        return remote(part, mr.at[g], m_s.at[d], m_r.at[g], k, j)

    def a_copy(d):
        j = (g + d) % ng
        part = mfull.at[pl.ds(pl.multiple_of(g * piece, 8), piece)]
        return remote(part, part, a_s.at[d], a_r.at[g], k, j)

    def m_partial():
        shift.wait_recv()
        mp[...] = jnp.dot(lt[...], nv[...].reshape(2 * rows, bands), preferred_element_type=F32)
        for d in range(1, ng):
            m_copy(d).start()

    def m_sum():
        own = pl.ds(pl.multiple_of(g * piece, 8), piece)
        total = mp[own]
        for d in range(1, ng):
            s = (g + d) % ng
            remote(mr.at[s], mr.at[s], m_s.at[d], m_r.at[s], k, s).wait_recv()
            total = total + mr[s]
        mfull[own] = total
        for d in range(1, ng):
            a_copy(d).start()

    def q_copies(i):
        return (
            remote(qs.at[i], qr.at[i], q_s.at[0, i], q_r.at[0, i], k, mate),
            remote(scs.at[i], scr.at[i], q_s.at[1, i], q_r.at[1, i], k, mate),
        )

    def q_start(i):
        for copy in q_copies(i):
            copy.start()

    def q2_copies(d):
        i = (pair + d) % pairs
        j = 2 * i + side
        return (
            remote(qs2.at[i], qr2.at[pair], q2_s.at[0, i], q2_r.at[0, pair], k, j),
            remote(scs2.at[i], scr2.at[pair], q2_s.at[1, i], q2_r.at[1, pair], k, j),
        )

    def encode(value, code_ref, scale_ref, i, which):
        top = jnp.maximum(jnp.max(jnp.abs(value), axis=0, keepdims=True), 1e-30)
        coded = jnp.round(value * (32767.0 / top)).astype(jnp.int32)
        code_ref[i, which] = coded.astype(jnp.int16)
        scale_ref[i, which] = jnp.broadcast_to(top * (1.0 / 32767.0), (8, share))

    def decode(code_ref, scale_ref, i, which):
        return code_ref[i, which].astype(jnp.int32).astype(F32) * scale_ref[i, which][0:1]

    def q_arrive(i):
        remote(qr.at[i], qr.at[i], q_s.at[0, i], q_r.at[0, i], k, mate).wait_recv()
        remote(scr.at[i], scr.at[i], q_s.at[1, i], q_r.at[1, i], k, mate).wait_recv()

    def q_second():
        for d in range(1, pairs):
            i = (pair + d) % pairs
            q_arrive(i)
            for which in range(2):
                encode(own[i, which] + decode(qr, scr, i, which), qs2, scs2, i, which)
            for copy in q2_copies(d):
                copy.start()

    @pl.when(even)
    def _():
        m_partial()

    def product(j, which):
        load(j, which).wait()
        table = pv[2 * j + which].reshape(2 * rows, share)
        return jnp.dot(lt[...], table, preferred_element_type=F32)

    def project_mate(i, carry):
        for which in range(2):
            encode(product(2 * i + 1 - side, which), qs, scs, i, which)

        @pl.when(odd)
        def _():
            q_start(i)
        return carry

    def project_own(i, carry):
        for which in range(2):
            own[i, which] = product(2 * i + side, which)
        return carry

    lax.fori_loop(0, pairs, project_mate, 0)
    lax.fori_loop(0, pairs, project_own, 0)

    @pl.when(even)
    def _():
        m_sum()
        for i in range(pairs):
            q_start(i)

    @pl.when(k == nk - 1)
    def _():
        local = map_ref[...] % rows
        both = jnp.concatenate([cv[0], cv[1]], axis=1)

        def permute(i, carry):
            ids = lax.broadcasted_iota(jnp.int32, (128, rows), 0) + i * 128
            pick = jnp.where(ids == local, 1.0, 0.0).astype(BF16)
            moved = jnp.dot(pick, both, preferred_element_type=F32).astype(BF16)
            at = pl.ds(pl.multiple_of(i * 128, 128), 128)
            for half in range(2):
                block = moved[:, half * bands:(half + 1) * bands].T
                here = pl.ds(pl.multiple_of(half * rows + i * 128, 128), 128)
                there = pl.ds(pl.multiple_of((1 - half) * rows + i * 128, 128), 128)
                lt[0:bands, here] = block
                lt[bands:, there] = block if half == 1 else -block
            return carry

        lax.fori_loop(0, rows // 128, permute, 0)

    @pl.when(odd)
    def _():
        m_partial()
        m_sum()
        q_second()

    for d in range(1, ng):
        s = (g + d) % ng
        part = mfull.at[pl.ds(pl.multiple_of(s * piece, 8), piece)]
        remote(part, part, a_s.at[d], a_r.at[s], k, s).wait_recv()

    mre = mfull[0:bands]
    mim = -mfull[bands:]
    diagonal = lax.broadcasted_iota(jnp.int32, (bands, bands), 0) == lax.broadcasted_iota(
        jnp.int32, (bands, bands), 1
    )
    two = jnp.where(diagonal, 2.0, 0.0).astype(F32)
    xr, xi = two - mre, -mim
    for newton_step in range(NEWTON - 1):
        yr, yi = cmul(mre, mim, xr, xi)
        xr, xi = cmul(xr, xi, two - yr, -yi)
    tb[0, 0] = xr
    tb[0, 1] = xi

    @pl.when(even)
    def _():
        if nk > 1:
            remote(tb.at[0], rb.at[0], x_s.at[0, 0], x_r.at[0, 0], k + 1, g).start()
        q_second()

    step = 0
    width = 1
    while width < nk:
        now, later = tb.at[step], tb.at[step + 1]
        spot = k % (2 * width)
        is_source = spot == width - 1
        is_target = spot >= width
        if width == 1:
            copy = remote(now, rb.at[step], x_s.at[step, 0], x_r.at[step, 0], (k + 1) % nk, g)

            @pl.when(is_source)
            def _():
                copy.wait_send()

            @pl.when(is_target)
            def _():
                copy.wait_recv()
        else:
            far = [
                remote(now.at[d % 2], rb.at[step, d % 2], x_s.at[step, d], x_r.at[step, 0], (k + 1 + d) % nk, g)
                for d in range(width)
            ]

            @pl.when(is_source)
            def _():
                for copy in far:
                    copy.start()

            def swap(half, partner):
                mine = rb.at[step, half]
                far[half].wait_recv()
                copy = remote(mine, mine, x_s.at[step, 0], x_r.at[step, 1], partner, g)
                copy.start()
                other = rb.at[step, 1 - half]
                remote(other, other, x_s.at[step, 0], x_r.at[step, 1], partner, g).wait_recv()
                copy.wait_send()

            @pl.when(jnp.logical_and(is_target, even))
            def _():
                swap(0, (k + 1) % nk)

            @pl.when(jnp.logical_and(is_target, odd))
            def _():
                swap(1, (k + nk - 1) % nk)

            @pl.when(is_source)
            def _():
                for copy in far:
                    copy.wait_send()

        @pl.when(is_target)
        def _():
            vr, vi = cmul(rb[step, 0], rb[step, 1], now[0], now[1])
            later[0] = vr
            later[1] = vi

        @pl.when(jnp.logical_not(is_target))
        def _():
            later[...] = now[...]

        step += 1
        width *= 2

    tr, ti = tb[step, 0], tb[step, 1]
    t_out[0, 0] = tr
    t_out[0, 1] = ti

    q_arrive(pair)
    sums = [own[pair, which] + decode(qr, scr, pair, which) for which in range(2)]
    for d in range(1, pairs):
        i = (pair + d) % pairs
        j = 2 * i + side
        remote(qr2.at[i], qr2.at[i], q2_s.at[0, i], q2_r.at[0, i], k, j).wait_recv()
        remote(scr2.at[i], scr2.at[i], q2_s.at[1, i], q2_r.at[1, i], k, j).wait_recv()
        for which in range(2):
            sums[which] = sums[which] + decode(qr2, scr2, i, which)
    br, bi = sums[0][0:bands], sums[0][bands:]
    dr, di = sums[1][0:bands], sums[1][bands:]
    wr, wi = cmul(tr.T, ti.T, br, bi)
    fp = jnp.sum(dr * wi - di * wr, axis=0, keepdims=True) * (1.0 / nk)
    atoms = atom_ref[pl.ds(g, 1), :]
    onehot = (lax.broadcasted_iota(jnp.int32, (NA, share), 0) == atoms).astype(F32)
    force = lax.dot_general(
        jnp.broadcast_to(fp, (8, share)), onehot, (((1,), (1,)), ((), ())),
        precision=lax.Precision.HIGHEST, preferred_element_type=F32,
    )

    fk[pl.ds(k, 1)] = force[None]
    for d in range(1, nk):
        remote(fk.at[k], fk.at[k], f_s.at[d], f_r.at[k], (k + d) % nk, g).start()
    for d in range(1, nk):
        s = (k + d) % nk
        remote(fk.at[s], fk.at[s], f_s.at[d], f_r.at[s], s, g).wait_recv()
    total = fk[0]
    for s in range(1, nk):
        total = total + fk[s]
    fg[pl.ds(g, 1)] = total[None]
    for d in range(1, ng):
        remote(fg.at[g], fg.at[g], g_s.at[d], g_r.at[g], k, (g + d) % ng).start()
    for d in range(1, ng):
        s = (g + d) % ng
        remote(fg.at[s], fg.at[s], g_s.at[d], g_r.at[s], k, s).wait_recv()
    total = fg[0]
    for s in range(1, ng):
        total = total + fg[s]
    f_out[...] = total

    shift.wait_send()
    for i in range(pairs):
        for copy in q_copies(i):
            copy.wait_send()
    for d in range(1, pairs):
        for copy in q2_copies(d):
            copy.wait_send()
    for d in range(1, ng):
        m_copy(d).wait_send()
        a_copy(d).wait_send()
        remote(fg.at[g], fg.at[g], g_s.at[d], g_r.at[g], k, (g + d) % ng).wait_send()
    for d in range(1, nk):
        remote(fk.at[k], fk.at[k], f_s.at[d], f_r.at[k], (k + d) % nk, g).wait_send()


def local(coeffs, projectors, proj_deriv, shift_map, atom_of):
    nk, ng = lax.axis_size("ka"), lax.axis_size("ga")
    rows, bands = coeffs.shape[2:]
    count = projectors.shape[2]
    share = count // ng
    steps = max(nk - 1, 1).bit_length()
    dma = pltpu.SemaphoreType.DMA
    vm = pl.BlockSpec(memory_space=pltpu.VMEM)
    hbm = pl.BlockSpec(memory_space=pl.ANY)
    transport, forces = pl.pallas_call(
        functools.partial(kernel, nk, ng),
        out_shape=(
            jax.ShapeDtypeStruct((1, 2, bands, bands), F32),
            jax.ShapeDtypeStruct((8, NA), F32),
        ),
        in_specs=[hbm, hbm, hbm, vm, vm],
        out_specs=(vm, vm),
        scratch_shapes=[
            pltpu.VMEM((2, rows, bands), BF16),
            pltpu.VMEM((2, rows, bands), BF16),
            pltpu.VMEM((2 * ng, 2, rows, share), BF16),
            pltpu.VMEM((2 * bands, 2 * rows), BF16),
            pltpu.VMEM((2 * bands, bands), F32),
            pltpu.VMEM((ng, 2 * bands // ng, bands), F32),
            pltpu.VMEM((2 * bands, bands), F32),
            *[
                pltpu.VMEM(shape, kind)
                for shape, kind in (
                    ((ng // 2, 2, 2 * bands, share), jnp.int16),
                    ((ng // 2, 2, 8, share), F32),
                )
                * 4
            ],
            pltpu.VMEM((ng // 2, 2, 2 * bands, share), F32),
            pltpu.VMEM((steps + 1, 2, bands, bands), F32),
            pltpu.VMEM((steps, 2, bands, bands), F32),
            pltpu.VMEM((nk, 8, NA), F32),
            pltpu.VMEM((ng, 8, NA), F32),
            dma, dma((2 * ng,)), dma, dma,
            dma((ng,)), dma((ng,)), dma((ng,)), dma((ng,)),
            *[dma((2, ng // 2))] * 4,
            dma((steps, max(nk // 2, 2))), dma((steps, 2)),
            dma((nk,)), dma((nk,)), dma((ng,)), dma((ng,)),
        ],
        compiler_params=pltpu.CompilerParams(
            collective_id=0, has_side_effects=True, vmem_limit_bytes=60 * 1024 * 1024
        ),
    )(coeffs, projectors, proj_deriv, shift_map.reshape(1, rows), atom_of.reshape(ng, share))
    return transport, forces[0]


def solution(mesh):
    placed = (P("ka", None, "ga", None), P(None, "ga", None), P(None, "ga", None), P("ga"), P())
    return jax.shard_map(
        local,
        mesh=mesh,
        in_specs=placed,
        out_specs=(P("ka", None, None, None), P()),
        check_vma=False,
    )
```
